8 devices in a mesh: dp: 1 (over z), tp: 2 (over y), pp: 4 (over x, core).
Axes of the slice: x: 2, y: 2, z: 1, core: 2. Of those that a mesh axis runs over, the one named last changes fastest.
Arguments:
- acts_in: bfloat16 [4, 1, 1536, 2560], P(None, 'dp')
- layer_kind: int32 [4, 1], P('pp')
- w_q: bfloat16 [4, 1, 2560, 2048], P('pp', None, None, 'tp')
- w_k: bfloat16 [4, 1, 2560, 1024], P('pp', None, None, 'tp')
- w_v: bfloat16 [4, 1, 2560, 1024], P('pp', None, None, 'tp')
- w_o: bfloat16 [4, 1, 2048, 2560], P('pp', None, 'tp')
- w_gate: bfloat16 [4, 1, 2560, 10240], P('pp', None, None, 'tp')
- w_up: bfloat16 [4, 1, 2560, 10240], P('pp', None, None, 'tp')
- w_down: bfloat16 [4, 1, 10240, 2560], P('pp', None, 'tp')
- norm_gains: float32 [4, 1, 4, 2560], P('pp')
- qk_gains: float32 [4, 1, 2, 256], P('pp')
Outputs:
- output: bfloat16 [4, 1, 1536, 2560], P(None, 'dp', 'pp')
All inputs are finite; a program needn't handle non-finite values.
Results may differ from the reference program's by a relative error of at most 0.02.
Values are sent between devices in bfloat16 or wider.
A program may use at most 1 GiB of HBM per device.

```python
import jax
import jax.numpy as jnp
from jax import lax

STAGES = 4
LAYERS = 1
MICRO = 4
BATCH = 1
SEQ = 1536
DMODEL = 2560
HEADS = 8
KV_HEADS = 4
HEAD_DIM = 256
FFN = 10240
WINDOW = 1024
QBLOCK = 256
MLP_ROWS = 512

GLOB_MIN = min(1, LAYERS - 1)
QUERY_PRE = DMODEL // HEADS if HEAD_DIM == 128 else HEAD_DIM
Q_SCALE = QUERY_PRE ** -0.5
GROUP_SIZE = HEADS // KV_HEADS
EPS = 1e-6
LOCAL_BASE = 10000.0
GLOBAL_BASE = 1000000.0
GLOBAL_POS_SCALE = 0.125


def draw_kind(kind_key):
    key_a, key_b, key_c = jax.random.split(kind_key, 3)
    extra_one = jax.random.randint(key_a, (STAGES,), 0, 2)
    stage_order = jax.random.permutation(key_b, STAGES)
    extra_one = extra_one.at[stage_order[0]].set(1).at[stage_order[1]].set(0)
    row_keys = jax.random.split(key_c, STAGES)
    layer_rank = jax.vmap(lambda sub_key: jax.random.permutation(sub_key, LAYERS))(row_keys)
    return (layer_rank < (GLOB_MIN + extra_one)[:, None]).astype(jnp.int32)


def dense_init(init_key, fan_in, dims_out):
    return (jax.random.normal(init_key, dims_out, jnp.float32) * fan_in ** -0.5).astype(jnp.bfloat16)


def setup_inputs(seed: int = 0, part: int = 0) -> dict:
    key_list = jax.random.split(jax.random.key(seed), 10)
    acts_key = jax.random.fold_in(jax.random.key(seed + 1), part)
    lead_dims = (STAGES, LAYERS)
    acts_in = jax.random.normal(acts_key, (MICRO, BATCH, SEQ, DMODEL), jnp.float32).astype(jnp.bfloat16)
    return dict(
        acts_in=acts_in,
        layer_kind=draw_kind(key_list[0]),
        w_q=dense_init(key_list[1], DMODEL, lead_dims + (DMODEL, HEADS * HEAD_DIM)),
        w_k=dense_init(key_list[2], DMODEL, lead_dims + (DMODEL, KV_HEADS * HEAD_DIM)),
        w_v=dense_init(key_list[3], DMODEL, lead_dims + (DMODEL, KV_HEADS * HEAD_DIM)),
        w_o=dense_init(key_list[4], HEADS * HEAD_DIM, lead_dims + (HEADS * HEAD_DIM, DMODEL)),
        w_gate=dense_init(key_list[5], DMODEL, lead_dims + (DMODEL, FFN)),
        w_up=dense_init(key_list[6], DMODEL, lead_dims + (DMODEL, FFN)),
        w_down=dense_init(key_list[7], FFN, lead_dims + (FFN, DMODEL)),
        norm_gains=0.3 * jax.random.normal(key_list[8], lead_dims + (4, DMODEL), jnp.float32),
        qk_gains=0.3 * jax.random.normal(key_list[9], lead_dims + (2, HEAD_DIM), jnp.float32),
    )


def rms_norm(x, gain_vec):
    x_f32 = x.astype(jnp.float32)
    mean_sq = jnp.mean(x_f32 * x_f32, axis=-1, keepdims=True)
    return (x_f32 * lax.rsqrt(mean_sq + EPS) * (1.0 + gain_vec)).astype(jnp.bfloat16)


def rope_tables(kind_val):
    is_glob = kind_val == 1
    expo_vec = jnp.arange(HEAD_DIM // 2, dtype=jnp.float32) * (-2.0 / HEAD_DIM)
    inv_freq = jnp.power(jnp.where(is_glob, GLOBAL_BASE, LOCAL_BASE).astype(jnp.float32), expo_vec)
    positions = jnp.arange(SEQ, dtype=jnp.float32) * jnp.where(is_glob, GLOBAL_POS_SCALE, 1.0).astype(jnp.float32)
    angles = positions[:, None] * inv_freq[None, :]
    return jnp.cos(angles), jnp.sin(angles)


def norm_rope(heads_in, gain_vec, cos_tab, sin_tab):
    x_f32 = heads_in.astype(jnp.float32)
    mean_sq = jnp.mean(x_f32 * x_f32, axis=-1, keepdims=True)
    x_f32 = x_f32 * lax.rsqrt(mean_sq + EPS) * (1.0 + gain_vec)
    half_dim = heads_in.shape[-1] // 2
    cos_b = cos_tab[None, :, None, :]
    sin_b = sin_tab[None, :, None, :]
    lo_half = x_f32[..., :half_dim]
    hi_half = x_f32[..., half_dim:]
    return jnp.concatenate([lo_half * cos_b - hi_half * sin_b, hi_half * cos_b + lo_half * sin_b], axis=-1).astype(jnp.bfloat16)


def attend_block(q_blk, k_win, v_win, q_pos, k_pos, span_max):
    scores = jnp.einsum('bqkgd,btkd->bkgqt', q_blk.astype(jnp.float32), k_win.astype(jnp.float32)) * Q_SCALE
    q_minus_k = q_pos[:, None] - k_pos[None, :]
    allowed = (q_minus_k >= 0) & (q_minus_k < span_max)
    scores = jnp.where(allowed, scores, -1e30)
    row_max = jnp.max(scores, axis=-1, keepdims=True)
    exp_val = jnp.exp(scores - row_max)
    prob_bf = (exp_val / jnp.sum(exp_val, axis=-1, keepdims=True)).astype(jnp.bfloat16)
    blk_out = jnp.einsum('bkgqt,btkd->bqkgd', prob_bf.astype(jnp.float32), v_win.astype(jnp.float32))
    return blk_out.astype(jnp.bfloat16)


def attention(q_rot, k_rot, v_heads, kind_val):
    win_len = WINDOW + QBLOCK
    blk_list = jnp.arange(SEQ // QBLOCK)

    def glob_block(blk_idx):
        q_start = blk_idx * QBLOCK
        q_blk = lax.dynamic_slice_in_dim(q_rot, q_start, QBLOCK, axis=1)
        q_pos = q_start + jnp.arange(QBLOCK)
        return attend_block(q_blk, k_rot, v_heads, q_pos, jnp.arange(SEQ), SEQ)

    def loc_block(blk_idx):
        q_start = blk_idx * QBLOCK
        q_blk = lax.dynamic_slice_in_dim(q_rot, q_start, QBLOCK, axis=1)
        q_pos = q_start + jnp.arange(QBLOCK)
        k_start = jnp.maximum(q_start - WINDOW, 0)
        k_win = lax.dynamic_slice_in_dim(k_rot, k_start, win_len, axis=1)
        v_win = lax.dynamic_slice_in_dim(v_heads, k_start, win_len, axis=1)
        return attend_block(q_blk, k_win, v_win, q_pos, k_start + jnp.arange(win_len), WINDOW)

    blocks = lax.cond(kind_val == 1, lambda ids_in: lax.map(glob_block, ids_in), lambda ids_in: lax.map(loc_block, ids_in), blk_list)
    return jnp.moveaxis(blocks, 0, 1).reshape(q_rot.shape)


def mlp_block(h_rows, w_gate, w_up, w_down):
    gate_f = jnp.dot(h_rows, w_gate, preferred_element_type=jnp.float32)
    up_f = jnp.dot(h_rows, w_up, preferred_element_type=jnp.float32)
    act_bf = (jax.nn.gelu(gate_f, approximate=True) * up_f).astype(jnp.bfloat16)
    return jnp.dot(act_bf, w_down, preferred_element_type=jnp.float32).astype(jnp.bfloat16)


def layer_fwd(hidden, params):
    w_q, w_k, w_v, w_o, w_gate, w_up, w_down, norm_gains, qk_gains, kind_val = params
    h_in = rms_norm(hidden, norm_gains[0]).reshape(BATCH * SEQ, DMODEL)
    q_proj = jnp.dot(h_in, w_q, preferred_element_type=jnp.float32).astype(jnp.bfloat16)
    k_proj = jnp.dot(h_in, w_k, preferred_element_type=jnp.float32).astype(jnp.bfloat16)
    v_proj = jnp.dot(h_in, w_v, preferred_element_type=jnp.float32).astype(jnp.bfloat16)
    cos_tab, sin_tab = rope_tables(kind_val)
    q_rot = norm_rope(q_proj.reshape(BATCH, SEQ, HEADS, HEAD_DIM), qk_gains[0], cos_tab, sin_tab)
    k_rot = norm_rope(k_proj.reshape(BATCH, SEQ, KV_HEADS, HEAD_DIM), qk_gains[1], cos_tab, sin_tab)
    q_rot = q_rot.reshape(BATCH, SEQ, KV_HEADS, GROUP_SIZE, HEAD_DIM)
    v_heads = v_proj.reshape(BATCH, SEQ, KV_HEADS, HEAD_DIM)
    attn_out = attention(q_rot, k_rot, v_heads, kind_val).reshape(BATCH * SEQ, HEADS * HEAD_DIM)
    o_proj = jnp.dot(attn_out, w_o, preferred_element_type=jnp.float32).astype(jnp.bfloat16).reshape(BATCH, SEQ, DMODEL)
    hidden = hidden + rms_norm(o_proj, norm_gains[1])
    h_mid = rms_norm(hidden, norm_gains[2]).reshape(BATCH * SEQ // MLP_ROWS, MLP_ROWS, DMODEL)
    d_out = lax.map(lambda rows_in: mlp_block(rows_in, w_gate, w_up, w_down), h_mid).reshape(BATCH, SEQ, DMODEL)
    return hidden + rms_norm(d_out, norm_gains[3])


def reference(acts_in, layer_kind, w_q, w_k, w_v, w_o, w_gate, w_up, w_down, norm_gains, qk_gains):
    stacked = tuple(arr_in.reshape((STAGES * LAYERS,) + arr_in.shape[2:]) for arr_in in (w_q, w_k, w_v, w_o, w_gate, w_up, w_down, norm_gains, qk_gains, layer_kind))

    def layer_step(hidden, params):
        return layer_fwd(hidden, params), None

    def one_micro(hidden):
        return lax.scan(layer_step, hidden, stacked)[0]

    return lax.map(one_micro, acts_in)
```

```python
import functools

import jax
import jax.numpy as jnp
from jax import lax
from jax.experimental import pallas as pl
from jax.experimental.pallas import tpu as pltpu
from jax.sharding import PartitionSpec as P


WINDOW = 1024
EPS = 1e-6
LOCAL_BASE = 10000.0
GLOBAL_BASE = 1000000.0
GLOBAL_POS_SCALE = 0.125
CHUNK = 192
LAG = 3
FTILE = 512
KSTEP = 256
NEG = -1e30


def rms_norm(x, gain_vec):
    x_f32 = x.astype(jnp.float32)
    mean_sq = jnp.mean(x_f32 * x_f32, axis=-1, keepdims=True)
    return (x_f32 * lax.rsqrt(mean_sq + EPS) * (1.0 + gain_vec)).astype(jnp.bfloat16)


def rope_tables(kind_val, seq_len, head_dim):
    is_glob = kind_val == 1
    expo_vec = jnp.arange(head_dim // 2, dtype=jnp.float32) * (-2.0 / head_dim)
    inv_freq = jnp.power(jnp.where(is_glob, GLOBAL_BASE, LOCAL_BASE).astype(jnp.float32), expo_vec)
    positions = jnp.arange(seq_len, dtype=jnp.float32) * jnp.where(is_glob, GLOBAL_POS_SCALE, 1.0).astype(jnp.float32)
    angles = positions[:, None] * inv_freq[None, :]
    return jnp.cos(angles), jnp.sin(angles)


def attn_kernel(meta, q_ref, k_ref, v_ref, kc_ref, vc_ref, cos_ref, sin_ref, gain_ref, o_ref, ko_ref, vo_ref, *, n_group, q_scale):
    chunk = meta[1]
    is_glob = meta[2] == 1
    head_dim = k_ref.shape[-1]
    half = head_dim // 2
    rows = k_ref.shape[0]
    cos_b = cos_ref[...]
    sin_b = sin_ref[...]

    def norm_rope(x, gain):
        x = x.astype(jnp.float32)
        mean_sq = jnp.mean(x * x, axis=-1, keepdims=True)
        x = x * lax.rsqrt(mean_sq + EPS) * (1.0 + gain)
        lo = x[:, :half]
        hi = x[:, half:]
        return jnp.concatenate([lo * cos_b - hi * sin_b, hi * cos_b + lo * sin_b], axis=-1).astype(jnp.bfloat16)

    k_new = norm_rope(k_ref[...], gain_ref[1:2, :])
    v_new = v_ref[...]
    ko_ref[0, 0] = k_new
    vo_ref[0, 0] = v_new
    q_all = jnp.concatenate([norm_rope(q_ref[:, g * head_dim:(g + 1) * head_dim], gain_ref[0:1, :]) for g in range(n_group)], axis=0)
    n_rows = n_group * rows
    start = chunk * rows
    span = jnp.where(is_glob, kc_ref.shape[2], WINDOW)
    first = jnp.where(is_glob, 0, jnp.maximum(start - WINDOW, 0))
    first = pl.multiple_of(first, 64)
    n_old = (start - first + KSTEP - 1) // KSTEP

    dims = (((1,), (1,)), ((), ()))
    dims_pv = (((1,), (0,)), ((), ()))
    s_new = lax.dot_general(q_all, k_new, dims, preferred_element_type=jnp.float32) * q_scale
    q_row = lax.rem(lax.broadcasted_iota(jnp.int32, (n_rows, rows), 0), rows)
    k_col = lax.broadcasted_iota(jnp.int32, (n_rows, rows), 1)
    s_new = jnp.where(k_col <= q_row, s_new, NEG)

    def emit(res):
        res = res.astype(jnp.bfloat16)
        for g in range(n_group):
            o_ref[:, g * head_dim:(g + 1) * head_dim] = res[g * rows:(g + 1) * rows]

    @pl.when(n_old == 0)
    def _():
        mx = jnp.max(s_new, axis=-1, keepdims=True)
        e_new = jnp.exp(s_new - mx)
        inv = 1.0 / jnp.sum(e_new, axis=-1, keepdims=True)
        emit(lax.dot_general((e_new * inv).astype(jnp.bfloat16), v_new, dims_pv, preferred_element_type=jnp.float32))

    def with_old(n):
        width = n * KSTEP
        k_old = kc_ref[0, 0, pl.ds(first, width), :]
        v_old = vc_ref[0, 0, pl.ds(first, width), :]
        s_old = lax.dot_general(q_all, k_old, dims, preferred_element_type=jnp.float32) * q_scale
        k_pos = first + lax.broadcasted_iota(jnp.int32, (n_rows, width), 1)
        q_pos = start + lax.rem(lax.broadcasted_iota(jnp.int32, (n_rows, width), 0), rows)
        s_old = jnp.where((k_pos < start) & (q_pos - k_pos < span), s_old, NEG)
        mx = jnp.maximum(jnp.max(s_new, axis=-1, keepdims=True), jnp.max(s_old, axis=-1, keepdims=True))
        e_new = jnp.exp(s_new - mx)
        e_old = jnp.exp(s_old - mx)
        inv = 1.0 / (jnp.sum(e_new, axis=-1, keepdims=True) + jnp.sum(e_old, axis=-1, keepdims=True))
        res = lax.dot_general((e_new * inv).astype(jnp.bfloat16), v_new, dims_pv, preferred_element_type=jnp.float32)
        res = res + lax.dot_general((e_old * inv).astype(jnp.bfloat16), v_old, dims_pv, preferred_element_type=jnp.float32)
        emit(res)

    for n in range(1, kc_ref.shape[2] // KSTEP + 1):
        pl.when(n_old == n)(functools.partial(with_old, n))


def attend(meta, qkv, k_cache, v_cache, cos_tab, sin_tab, gains, q_scale):
    rows = qkv.shape[0]
    _, kv_heads, seq_len, head_dim = k_cache.shape
    n_group = qkv.shape[1] // (kv_heads * head_dim) - 2
    q_cols = n_group * kv_heads
    cache_in = pl.BlockSpec((1, 1, seq_len, head_dim), lambda h, m: (m[0], h, 0, 0))
    cache_out = pl.BlockSpec((1, 1, rows, head_dim), lambda h, m: (m[0], h, m[1], 0))
    table = pl.BlockSpec((rows, head_dim // 2), lambda h, m: (m[1], 0))
    grid_spec = pltpu.PrefetchScalarGridSpec(
        num_scalar_prefetch=1,
        grid=(kv_heads,),
        in_specs=[
            pl.BlockSpec((rows, n_group * head_dim), lambda h, m: (0, h)),
            pl.BlockSpec((rows, head_dim), lambda h, m: (0, q_cols + h)),
            pl.BlockSpec((rows, head_dim), lambda h, m: (0, q_cols + kv_heads + h)),
            cache_in,
            cache_in,
            table,
            table,
            pl.BlockSpec((2, head_dim), lambda h, m: (0, 0)),
        ],
        out_specs=[pl.BlockSpec((rows, n_group * head_dim), lambda h, m: (0, h)), cache_out, cache_out],
    )
    flops = 4 * rows * q_cols * head_dim * 900
    return pl.pallas_call(
        functools.partial(attn_kernel, n_group=n_group, q_scale=q_scale),
        grid_spec=grid_spec,
        out_shape=[
            jax.ShapeDtypeStruct((rows, q_cols * head_dim), jnp.bfloat16),
            jax.ShapeDtypeStruct(k_cache.shape, k_cache.dtype),
            jax.ShapeDtypeStruct(v_cache.shape, v_cache.dtype),
        ],
        input_output_aliases={4: 1, 5: 2},
        compiler_params=pltpu.CompilerParams(vmem_limit_bytes=32 * 2**20, dimension_semantics=("arbitrary",)),
        cost_estimate=pl.CostEstimate(flops=flops, bytes_accessed=8 * 2**20, transcendentals=0),
        name="attend",
    )(meta, qkv, qkv, qkv, k_cache, v_cache, cos_tab, sin_tab, gains)


def mlp_kernel(uo_ref, ux_ref, wg_ref, wu_ref, wd_ref, do_ref, dx_ref, u_all, acc, act):
    step = pl.program_id(0)
    last = pl.num_programs(0) - 1
    rows = uo_ref.shape[0]

    def gate_up():
        gate = jnp.dot(u_all[...], wg_ref[...], preferred_element_type=jnp.float32)
        up = jnp.dot(u_all[...], wu_ref[...], preferred_element_type=jnp.float32)
        return (jax.nn.gelu(gate, approximate=True) * up).astype(jnp.bfloat16)

    def down():
        return jnp.dot(act[...], wd_ref[...], preferred_element_type=jnp.float32)

    @pl.when(step == 0)
    def _():
        u_all[:rows] = uo_ref[...]
        u_all[rows:] = ux_ref[...]
        acc[...] = jnp.zeros_like(acc)
        act[...] = gate_up()

    @pl.when((step > 0) & (step < last))
    def _():
        acc[...] += down()
        act[...] = gate_up()

    @pl.when(step == last)
    def _():
        res = acc[...] + down()
        do_ref[...] = res[:rows]
        dx_ref[...] = res[rows:].astype(jnp.bfloat16)


def mlp(u_own, u_oth, w_gate, w_up, w_down):
    rows, d_model = u_own.shape
    ffn = w_gate.shape[1]
    n_tiles = ffn // FTILE
    whole = pl.BlockSpec((rows, d_model), lambda f: (0, 0))
    col = pl.BlockSpec((d_model, FTILE), lambda f: (0, jnp.minimum(f, n_tiles - 1)))
    row = pl.BlockSpec((FTILE, d_model), lambda f: (jnp.maximum(f - 1, 0), 0))
    return pl.pallas_call(
        mlp_kernel,
        grid=(n_tiles + 1,),
        in_specs=[whole, whole, col, col, row],
        out_specs=[whole, whole],
        out_shape=[jax.ShapeDtypeStruct((rows, d_model), jnp.float32), jax.ShapeDtypeStruct((rows, d_model), jnp.bfloat16)],
        scratch_shapes=[
            pltpu.VMEM((2 * rows, d_model), jnp.bfloat16),
            pltpu.VMEM((2 * rows, d_model), jnp.float32),
            pltpu.VMEM((2 * rows, FTILE), jnp.bfloat16),
        ],
        compiler_params=pltpu.CompilerParams(vmem_limit_bytes=40 * 2**20, dimension_semantics=("arbitrary",)),
        cost_estimate=pl.CostEstimate(flops=12 * rows * d_model * ffn, bytes_accessed=6 * d_model * ffn, transcendentals=0),
        name="mlp",
    )(u_own, u_oth, w_gate, w_up, w_down)


def solution(mesh):
    n_stages = mesh.shape['pp']
    last_stage = n_stages - 1
    col_split = P('pp', None, None, 'tp')
    row_split = P('pp', None, 'tp', None)
    stage_only = P('pp', None, None, None)
    in_specs = (P(None, 'dp', None, None), P('pp', None), col_split, col_split, col_split, row_split, col_split, col_split, row_split, stage_only, stage_only)
    out_spec = P(None, 'dp', 'pp', None)
    axes = ('tp', 'pp')

    def dev(t, s):
        return t * n_stages + s

    def run_all(acts_in, layer_kind, w_q, w_k, w_v, w_o, w_gate, w_up, w_down, norm_gains, qk_gains):
        head_dim = qk_gains.shape[-1]
        q_heads = w_q.shape[-1] // head_dim
        query_pre = acts_in.shape[-1] // q_heads if head_dim == 128 else head_dim
        q_scale = query_pre ** -0.5

        def device_fn(acts_loc, kind_loc, wq_loc, wk_loc, wv_loc, wo_loc, wg_loc, wu_loc, wd_loc, gain_loc, qk_loc):
            side = lax.axis_index('tp')
            stage = lax.axis_index('pp')
            at_first = stage == 0
            n_micro, _, seq_len, d_model = acts_loc.shape
            n_own = n_micro // 2
            n_chunks = seq_len // CHUNK
            n_units = n_own * n_chunks
            kv_heads = wk_loc.shape[-1] // head_dim
            kind_val = kind_loc[0, 0]
            gains = gain_loc[0, 0]
            qk_gain = qk_loc[0, 0]
            w_gate, w_up, w_down = wg_loc[0, 0], wu_loc[0, 0], wd_loc[0, 0]
            f32 = jnp.float32

            def swap(x, stages):
                pairs = [(dev(t, s), dev(1 - t, s)) for s in stages for t in (0, 1)]
                return lax.ppermute(x, axes, pairs)

            wqkv_own = jnp.concatenate([wq_loc[0, 0], wk_loc[0, 0], wv_loc[0, 0]], axis=1)
            wo_own = wo_loc[0, 0]
            later = range(1, n_stages)
            wqkv_oth = jnp.where(at_first, wqkv_own, swap(wqkv_own, later))
            wo_oth = jnp.where(at_first, wo_own, swap(wo_own, later))
            fill = LAG - 1
            cos_tab, sin_tab = rope_tables(kind_val, seq_len, head_dim)
            caches = [jnp.zeros((n_own, kv_heads, seq_len, head_dim), jnp.bfloat16) for _ in range(4)]

            def active(slot):
                return [s for s in range(n_stages) if 0 <= slot - LAG * s < n_units]

            n_slots = n_units + LAG * last_stage
            x_recv, x_mid, u_own, u_oth, d_own, d_oth = {}, {}, {}, {}, {}, {}
            pieces = {}
            for slot in range(n_slots + 2):
                if slot < n_slots:
                    unit = jnp.clip(slot - LAG * stage, 0, n_units - 1)
                    meta = jnp.stack([unit % n_own, unit // n_own, kind_val]).astype(jnp.int32)
                    if slot < n_units:
                        row0 = (slot // n_own) * CHUNK
                        at_own = (side * n_own + slot % n_own, 0, row0, 0)
                        at_oth = ((1 - side) * n_own + slot % n_own, 0, row0, 0)
                        size = (1, 1, CHUNK, d_model)
                        x_own = lax.dynamic_slice(acts_loc, at_own, size).reshape(CHUNK, d_model)
                        x_two = lax.dynamic_slice(acts_loc, at_oth, size).reshape(CHUNK, d_model)
                        if slot >= LAG:
                            x_own = jnp.where(at_first, x_own, x_recv[slot])
                            x_two = jnp.where(at_first, x_two, x_recv[slot])
                    else:
                        x_own = x_two = x_recv[slot]
                    if slot >= 2:
                        x_own, x_two, _ = lax.optimization_barrier((x_own, x_two, d_own[slot - 2]))
                    h_own = rms_norm(x_own, gains[0])
                    h_two = rms_norm(x_two, gains[0]) if slot < n_units else h_own
                    qkv_a = jnp.dot(h_own, wqkv_own, preferred_element_type=f32).astype(jnp.bfloat16)
                    wqkv_two, wo_two = (wqkv_oth, wo_oth) if slot > fill else (wqkv_own, wo_own)
                    qkv_b = jnp.dot(h_two, wqkv_two, preferred_element_type=f32).astype(jnp.bfloat16)
                    att_a, caches[0], caches[1] = attend(meta, qkv_a, caches[0], caches[1], cos_tab, sin_tab, qk_gain, q_scale)
                    att_b, caches[2], caches[3] = attend(meta, qkv_b, caches[2], caches[3], cos_tab, sin_tab, qk_gain, q_scale)
                    o_b = jnp.dot(att_b, wo_two, preferred_element_type=f32)
                    if slot < n_units:
                        o_b = jnp.where(at_first, swap(o_b.astype(jnp.bfloat16), [0]).astype(f32), o_b)
                    o_sum = (jnp.dot(att_a, wo_own, preferred_element_type=f32) + o_b).astype(jnp.bfloat16)
                    x_mid[slot] = x_own + rms_norm(o_sum, gains[1])
                    u_own[slot] = rms_norm(x_mid[slot], gains[2])
                    u_oth[slot] = swap(u_own[slot], active(slot))
                x_out = None
                if 0 <= slot - 2 < n_slots:
                    done = slot - 2
                    d_sum = (d_own[done] + d_oth[done].astype(f32)).astype(jnp.bfloat16)
                    x_out = x_mid[done] + rms_norm(d_sum, gains[3])
                    movers = [s for s in active(done) if s < last_stage]
                    if movers:
                        x_recv[done + LAG] = lax.ppermute(x_out, 'pp', [(s, s + 1) for s in movers])
                    out_unit = done - LAG * last_stage
                    if out_unit >= 0:
                        stream, chunk = out_unit % n_own, out_unit // n_own
                        per = n_chunks // n_stages
                        target, part = chunk // per, chunk % per
                        if target == last_stage:
                            mine = jnp.where(stage == last_stage, x_out, jnp.zeros_like(x_out))
                        else:
                            mine = lax.ppermute(x_out, axes, [(dev(t, last_stage), dev(t, target)) for t in (0, 1)])
                        theirs = lax.ppermute(x_out, axes, [(dev(t, last_stage), dev(1 - t, target)) for t in (0, 1)])
                        for key, val in (((0, stream, part), mine), ((1, stream, part), theirs)):
                            pieces[key] = pieces[key] + val if key in pieces else val

                if 0 <= slot - 1 < n_slots:
                    prev = slot - 1
                    u_in = u_own[prev]
                    if slot < n_slots:
                        u_in = lax.optimization_barrier((u_in, u_own[slot]))[0]
                    if x_out is not None:
                        u_in = lax.optimization_barrier((u_in, x_out))[0]
                    d_own[prev], d_send = mlp(u_in, u_oth[prev], w_gate, w_up, w_down)
                    d_oth[prev] = swap(d_send, active(prev))

            per = n_chunks // n_stages
            mine = [jnp.concatenate([pieces[(0, m, r)] for r in range(per)], axis=0) for m in range(n_own)]
            theirs = [jnp.concatenate([pieces[(1, m, r)] for r in range(per)], axis=0) for m in range(n_own)]
            on_zero = side == 0
            out = [jnp.where(on_zero, a, b) for a, b in zip(mine, theirs)] + [jnp.where(on_zero, b, a) for a, b in zip(mine, theirs)]
            return jnp.stack(out)[:, None]

        return jax.shard_map(device_fn, mesh=mesh, in_specs=in_specs, out_specs=out_spec, check_vma=False)(acts_in, layer_kind, w_q, w_k, w_v, w_o, w_gate, w_up, w_down, norm_gains, qk_gains)

    return run_all
```

```python
import functools

import jax
import jax.numpy as jnp
from jax import lax
from jax.experimental import pallas as pl
from jax.experimental.pallas import tpu as pltpu
from jax.sharding import PartitionSpec as P


WINDOW = 1024
EPS = 1e-6
LOCAL_BASE = 10000.0
GLOBAL_BASE = 1000000.0
GLOBAL_POS_SCALE = 0.125
CHUNK = 192
LAG = 3
FTILE = 512
KSTEP = 256
NEG = -1e30


def rms_norm(x, gain_vec):
    x_f32 = x.astype(jnp.float32)
    mean_sq = jnp.mean(x_f32 * x_f32, axis=-1, keepdims=True)
    return (x_f32 * lax.rsqrt(mean_sq + EPS) * (1.0 + gain_vec)).astype(jnp.bfloat16)


def rope_tables(kind_val, seq_len, head_dim):
    is_glob = kind_val == 1
    expo_vec = jnp.arange(head_dim // 2, dtype=jnp.float32) * (-2.0 / head_dim)
    inv_freq = jnp.power(jnp.where(is_glob, GLOBAL_BASE, LOCAL_BASE).astype(jnp.float32), expo_vec)
    positions = jnp.arange(seq_len, dtype=jnp.float32) * jnp.where(is_glob, GLOBAL_POS_SCALE, 1.0).astype(jnp.float32)
    angles = positions[:, None] * inv_freq[None, :]
    return jnp.cos(angles), jnp.sin(angles)


def attn_kernel(meta, x_ref, w_ref, wo_ref, kc_ref, vc_ref, cos_ref, sin_ref, gain0_ref, gain_ref, o_ref, ko_ref, vo_ref, h_ref, acc, *, n_group, q_scale):
    head = pl.program_id(0)
    chunk = meta[1]
    is_glob = meta[2] == 1
    head_dim = ko_ref.shape[-1]
    half = head_dim // 2
    rows = x_ref.shape[0]
    n_rows = n_group * rows
    q_cols = n_group * head_dim
    cos_b = cos_ref[...]
    sin_b = sin_ref[...]

    @pl.when(head == 0)
    def _():
        x = x_ref[...].astype(jnp.float32)
        mean_sq = jnp.mean(x * x, axis=-1, keepdims=True)
        h_ref[...] = (x * lax.rsqrt(mean_sq + EPS) * (1.0 + gain0_ref[...])).astype(jnp.bfloat16)
        acc[...] = jnp.zeros_like(acc)

    def norm_rope(x, gain):
        x = x.astype(jnp.bfloat16).astype(jnp.float32)
        mean_sq = jnp.mean(x * x, axis=-1, keepdims=True)
        x = x * lax.rsqrt(mean_sq + EPS) * (1.0 + gain)
        lo = x[:, :half]
        hi = x[:, half:]
        return jnp.concatenate([lo * cos_b - hi * sin_b, hi * cos_b + lo * sin_b], axis=-1).astype(jnp.bfloat16)

    qkv = jnp.dot(h_ref[...], w_ref[...], preferred_element_type=jnp.float32)
    k_new = norm_rope(qkv[:, q_cols:q_cols + head_dim], gain_ref[1:2, :])
    v_new = qkv[:, q_cols + head_dim:].astype(jnp.bfloat16)
    ko_ref[0, 0] = k_new
    vo_ref[0, 0] = v_new
    q_all = jnp.concatenate([norm_rope(qkv[:, g * head_dim:(g + 1) * head_dim], gain_ref[0:1, :]) for g in range(n_group)], axis=0)
    start = chunk * rows
    span = jnp.where(is_glob, kc_ref.shape[2], WINDOW)
    first = jnp.where(is_glob, 0, jnp.maximum(start - WINDOW, 0))
    first = pl.multiple_of(first, 64)
    n_old = (start - first + KSTEP - 1) // KSTEP

    dims = (((1,), (1,)), ((), ()))
    dims_pv = (((1,), (0,)), ((), ()))
    s_new = lax.dot_general(q_all, k_new, dims, preferred_element_type=jnp.float32) * q_scale
    q_row = lax.rem(lax.broadcasted_iota(jnp.int32, (n_rows, rows), 0), rows)
    k_col = lax.broadcasted_iota(jnp.int32, (n_rows, rows), 1)
    s_new = jnp.where(k_col <= q_row, s_new, NEG)

    def emit(res):
        res = res.astype(jnp.bfloat16)
        att = jnp.concatenate([res[g * rows:(g + 1) * rows] for g in range(n_group)], axis=1)
        acc[...] += jnp.dot(att, wo_ref[...], preferred_element_type=jnp.float32)

    @pl.when(n_old == 0)
    def _():
        mx = jnp.max(s_new, axis=-1, keepdims=True)
        e_new = jnp.exp(s_new - mx)
        inv = 1.0 / jnp.sum(e_new, axis=-1, keepdims=True)
        emit(lax.dot_general((e_new * inv).astype(jnp.bfloat16), v_new, dims_pv, preferred_element_type=jnp.float32))

    def with_old(n):
        width = n * KSTEP
        k_old = kc_ref[0, 0, pl.ds(first, width), :]
        v_old = vc_ref[0, 0, pl.ds(first, width), :]
        s_old = lax.dot_general(q_all, k_old, dims, preferred_element_type=jnp.float32) * q_scale
        k_pos = first + lax.broadcasted_iota(jnp.int32, (n_rows, width), 1)
        q_pos = start + lax.rem(lax.broadcasted_iota(jnp.int32, (n_rows, width), 0), rows)
        s_old = jnp.where((k_pos < start) & (q_pos - k_pos < span), s_old, NEG)
        mx = jnp.maximum(jnp.max(s_new, axis=-1, keepdims=True), jnp.max(s_old, axis=-1, keepdims=True))
        e_new = jnp.exp(s_new - mx)
        e_old = jnp.exp(s_old - mx)
        inv = 1.0 / (jnp.sum(e_new, axis=-1, keepdims=True) + jnp.sum(e_old, axis=-1, keepdims=True))
        res = lax.dot_general((e_new * inv).astype(jnp.bfloat16), v_new, dims_pv, preferred_element_type=jnp.float32)
        res = res + lax.dot_general((e_old * inv).astype(jnp.bfloat16), v_old, dims_pv, preferred_element_type=jnp.float32)
        emit(res)

    for n in range(1, kc_ref.shape[2] // KSTEP + 1):
        pl.when(n_old == n)(functools.partial(with_old, n))

    @pl.when(head == pl.num_programs(0) - 1)
    def _():
        o_ref[...] = acc[...]


def attend(meta, x, w_qkv, w_o, k_cache, v_cache, cos_tab, sin_tab, gain0, gains, q_scale):
    rows, d_model = x.shape
    _, kv_heads, seq_len, head_dim = k_cache.shape
    cols = w_qkv.shape[1] // kv_heads
    n_group = cols // head_dim - 2
    cache_in = pl.BlockSpec((1, 1, seq_len, head_dim), lambda h, m: (m[0], h, 0, 0))
    cache_out = pl.BlockSpec((1, 1, rows, head_dim), lambda h, m: (m[0], h, m[1], 0))
    table = pl.BlockSpec((rows, head_dim // 2), lambda h, m: (m[1], 0))
    grid_spec = pltpu.PrefetchScalarGridSpec(
        num_scalar_prefetch=1,
        grid=(kv_heads,),
        in_specs=[
            pl.BlockSpec((rows, d_model), lambda h, m: (0, 0)),
            pl.BlockSpec((d_model, cols), lambda h, m: (0, h)),
            pl.BlockSpec((n_group * head_dim, d_model), lambda h, m: (h, 0)),
            cache_in,
            cache_in,
            table,
            table,
            pl.BlockSpec((1, d_model), lambda h, m: (0, 0)),
            pl.BlockSpec((2, head_dim), lambda h, m: (0, 0)),
        ],
        out_specs=[pl.BlockSpec((rows, d_model), lambda h, m: (0, 0)), cache_out, cache_out],
        scratch_shapes=[pltpu.VMEM((rows, d_model), jnp.bfloat16), pltpu.VMEM((rows, d_model), jnp.float32)],
    )
    flops = 2 * rows * d_model * (w_qkv.shape[1] + w_o.shape[0]) + 4 * rows * w_o.shape[0] * 900
    return pl.pallas_call(
        functools.partial(attn_kernel, n_group=n_group, q_scale=q_scale),
        grid_spec=grid_spec,
        out_shape=[
            jax.ShapeDtypeStruct((rows, d_model), jnp.float32),
            jax.ShapeDtypeStruct(k_cache.shape, k_cache.dtype),
            jax.ShapeDtypeStruct(v_cache.shape, v_cache.dtype),
        ],
        input_output_aliases={4: 1, 5: 2},
        compiler_params=pltpu.CompilerParams(vmem_limit_bytes=44 * 2**20, dimension_semantics=("arbitrary",)),
        cost_estimate=pl.CostEstimate(flops=flops, bytes_accessed=20 * 2**20, transcendentals=0),
        name="attend",
    )(meta, x, w_qkv, w_o, k_cache, v_cache, cos_tab, sin_tab, gain0, gains)


def mlp_kernel(uo_ref, ux_ref, wg_ref, wu_ref, wd_ref, do_ref, dx_ref, u_all, acc, act):
    step = pl.program_id(0)
    last = pl.num_programs(0) - 1
    rows = uo_ref.shape[0]

    def gate_up():
        gate = jnp.dot(u_all[...], wg_ref[...], preferred_element_type=jnp.float32)
        up = jnp.dot(u_all[...], wu_ref[...], preferred_element_type=jnp.float32)
        return (jax.nn.gelu(gate, approximate=True) * up).astype(jnp.bfloat16)

    def down():
        return jnp.dot(act[...], wd_ref[...], preferred_element_type=jnp.float32)

    @pl.when(step == 0)
    def _():
        u_all[:rows] = uo_ref[...]
        u_all[rows:] = ux_ref[...]
        acc[...] = jnp.zeros_like(acc)
        act[...] = gate_up()

    @pl.when((step > 0) & (step < last))
    def _():
        acc[...] += down()
        act[...] = gate_up()

    @pl.when(step == last)
    def _():
        res = acc[...] + down()
        do_ref[...] = res[:rows]
        dx_ref[...] = res[rows:].astype(jnp.bfloat16)


def mlp(u_own, u_oth, w_gate, w_up, w_down):
    rows, d_model = u_own.shape
    ffn = w_gate.shape[1]
    n_tiles = ffn // FTILE
    whole = pl.BlockSpec((rows, d_model), lambda f: (0, 0))
    col = pl.BlockSpec((d_model, FTILE), lambda f: (0, jnp.minimum(f, n_tiles - 1)))
    row = pl.BlockSpec((FTILE, d_model), lambda f: (jnp.maximum(f - 1, 0), 0))
    return pl.pallas_call(
        mlp_kernel,
        grid=(n_tiles + 1,),
        in_specs=[whole, whole, col, col, row],
        out_specs=[whole, whole],
        out_shape=[jax.ShapeDtypeStruct((rows, d_model), jnp.float32), jax.ShapeDtypeStruct((rows, d_model), jnp.bfloat16)],
        scratch_shapes=[
            pltpu.VMEM((2 * rows, d_model), jnp.bfloat16),
            pltpu.VMEM((2 * rows, d_model), jnp.float32),
            pltpu.VMEM((2 * rows, FTILE), jnp.bfloat16),
        ],
        compiler_params=pltpu.CompilerParams(vmem_limit_bytes=40 * 2**20, dimension_semantics=("arbitrary",)),
        cost_estimate=pl.CostEstimate(flops=12 * rows * d_model * ffn, bytes_accessed=6 * d_model * ffn, transcendentals=0),
        name="mlp",
    )(u_own, u_oth, w_gate, w_up, w_down)


def solution(mesh):
    n_stages = mesh.shape['pp']
    last_stage = n_stages - 1
    col_split = P('pp', None, None, 'tp')
    row_split = P('pp', None, 'tp', None)
    stage_only = P('pp', None, None, None)
    in_specs = (P(None, 'dp', None, None), P('pp', None), col_split, col_split, col_split, row_split, col_split, col_split, row_split, stage_only, stage_only)
    out_spec = P(None, 'dp', 'pp', None)
    axes = ('tp', 'pp')

    def dev(t, s):
        return t * n_stages + s

    def run_all(acts_in, layer_kind, w_q, w_k, w_v, w_o, w_gate, w_up, w_down, norm_gains, qk_gains):
        head_dim = qk_gains.shape[-1]
        q_heads = w_q.shape[-1] // head_dim
        query_pre = acts_in.shape[-1] // q_heads if head_dim == 128 else head_dim
        q_scale = query_pre ** -0.5

        def device_fn(acts_loc, kind_loc, wq_loc, wk_loc, wv_loc, wo_loc, wg_loc, wu_loc, wd_loc, gain_loc, qk_loc):
            side = lax.axis_index('tp')
            stage = lax.axis_index('pp')
            at_first = stage == 0
            n_micro, _, seq_len, d_model = acts_loc.shape
            n_own = n_micro // 2
            n_chunks = seq_len // CHUNK
            n_units = n_own * n_chunks
            kv_heads = wk_loc.shape[-1] // head_dim
            kind_val = kind_loc[0, 0]
            gains = gain_loc[0, 0]
            qk_gain = qk_loc[0, 0]
            w_gate, w_up, w_down = wg_loc[0, 0], wu_loc[0, 0], wd_loc[0, 0]
            f32 = jnp.float32

            def swap(x, stages):
                pairs = [(dev(t, s), dev(1 - t, s)) for s in stages for t in (0, 1)]
                return lax.ppermute(x, axes, pairs)

            n_group = q_heads // (w_k.shape[-1] // head_dim)
            groups = []
            for g in range(kv_heads):
                at_kv = slice(g * head_dim, (g + 1) * head_dim)
                groups += [wq_loc[0, 0][:, g * n_group * head_dim:(g + 1) * n_group * head_dim], wk_loc[0, 0][:, at_kv], wv_loc[0, 0][:, at_kv]]
            wqkv_own = jnp.concatenate(groups, axis=1)
            wo_own = wo_loc[0, 0]
            later = range(1, n_stages)
            wqkv_oth = jnp.where(at_first, wqkv_own, swap(wqkv_own, later))
            wo_oth = jnp.where(at_first, wo_own, swap(wo_own, later))
            fill = LAG - 1
            cos_tab, sin_tab = rope_tables(kind_val, seq_len, head_dim)
            caches = [jnp.zeros((n_own, kv_heads, seq_len, head_dim), jnp.bfloat16) for _ in range(4)]

            def active(slot):
                return [s for s in range(n_stages) if 0 <= slot - LAG * s < n_units]

            n_slots = n_units + LAG * last_stage
            x_recv, x_mid, u_own, u_oth, d_own, d_oth = {}, {}, {}, {}, {}, {}
            pieces = {}
            landed, landing = [], []
            for slot in range(n_slots + 2):
                if slot < n_slots:
                    unit = jnp.clip(slot - LAG * stage, 0, n_units - 1)
                    meta = jnp.stack([unit % n_own, unit // n_own, kind_val]).astype(jnp.int32)
                    if slot < n_units:
                        row0 = (slot // n_own) * CHUNK
                        at_own = (side * n_own + slot % n_own, 0, row0, 0)
                        at_oth = ((1 - side) * n_own + slot % n_own, 0, row0, 0)
                        size = (1, 1, CHUNK, d_model)
                        x_own = lax.dynamic_slice(acts_loc, at_own, size).reshape(CHUNK, d_model)
                        x_two = lax.dynamic_slice(acts_loc, at_oth, size).reshape(CHUNK, d_model)
                        if slot >= LAG:
                            x_got = lax.optimization_barrier((x_recv[slot], d_own[slot - 2]))[0]
                            x_own = jnp.where(at_first, x_own, x_got)
                            x_two = jnp.where(at_first, x_two, x_got)
                        elif slot >= 2:
                            x_own, x_two, _ = lax.optimization_barrier((x_own, x_two, d_own[slot - 2]))
                    else:
                        x_own = x_two = lax.optimization_barrier((x_recv[slot], d_own[slot - 2]))[0]
                    wqkv_two, wo_two = (wqkv_oth, wo_oth) if slot > fill else (wqkv_own, wo_own)
                    o_b, caches[2], caches[3] = attend(meta, x_two, wqkv_two, wo_two, caches[2], caches[3], cos_tab, sin_tab, gains[:1], qk_gain, q_scale)
                    if slot < n_units:
                        o_b = jnp.where(at_first, swap(o_b.astype(jnp.bfloat16), [0]).astype(f32), o_b)
                    o_a, caches[0], caches[1] = attend(meta, x_own, wqkv_own, wo_own, caches[0], caches[1], cos_tab, sin_tab, gains[:1], qk_gain, q_scale)
                    o_sum = (o_a + o_b).astype(jnp.bfloat16)
                    x_mid[slot] = x_own + rms_norm(o_sum, gains[1])
                    u_own[slot] = rms_norm(x_mid[slot], gains[2])
                    u_oth[slot] = swap(u_own[slot], active(slot))
                x_out = None
                if 0 <= slot - 2 < n_slots:
                    done = slot - 2
                    d_sum = (d_own[done] + d_oth[done].astype(f32)).astype(jnp.bfloat16)
                    x_out = x_mid[done] + rms_norm(d_sum, gains[3])
                    movers = [s for s in active(done) if s < last_stage]
                    if movers:
                        x_recv[done + LAG] = lax.ppermute(x_out, 'pp', [(s, s + 1) for s in movers])
                    out_unit = done - LAG * last_stage
                    if out_unit >= 0:
                        stream, chunk = out_unit % n_own, out_unit // n_own
                        per = n_chunks // n_stages
                        target, part = chunk // per, chunk % per
                        if target == last_stage:
                            mine = jnp.where(stage == last_stage, x_out, jnp.zeros_like(x_out))
                        else:
                            mine = lax.ppermute(x_out, axes, [(dev(t, last_stage), dev(t, target)) for t in (0, 1)])
                        theirs = lax.ppermute(x_out, axes, [(dev(t, last_stage), dev(1 - t, target)) for t in (0, 1)])
                        for key, val in (((0, stream, part), mine), ((1, stream, part), theirs)):
                            pieces.setdefault(key, []).append(val)
                        landing = [(0, stream, part), (1, stream, part)]

                if 0 <= slot - 1 < n_slots:
                    prev = slot - 1
                    u_in = u_own[prev]
                    if slot < n_slots:
                        u_in = lax.optimization_barrier((u_in, u_own[slot]))[0]
                    if x_out is not None:
                        u_in = lax.optimization_barrier((u_in, x_out))[0]
                    for key in landed:
                        *rest, newest = pieces[key]
                        u_in, newest = lax.optimization_barrier((u_in, newest))
                        pieces[key] = [sum(rest, newest)]
                    d_own[prev], d_send = mlp(u_in, u_oth[prev], w_gate, w_up, w_down)
                    d_oth[prev] = swap(d_send, active(prev))
                landed, landing = landing, []

            per = n_chunks // n_stages
            total = {key: sum(vals[1:], vals[0]) for key, vals in pieces.items()}
            mine = [jnp.concatenate([total[(0, m, r)] for r in range(per)], axis=0) for m in range(n_own)]
            theirs = [jnp.concatenate([total[(1, m, r)] for r in range(per)], axis=0) for m in range(n_own)]
            on_zero = side == 0
            out = [jnp.where(on_zero, a, b) for a, b in zip(mine, theirs)] + [jnp.where(on_zero, b, a) for a, b in zip(mine, theirs)]
            return jnp.stack(out)[:, None]

        return jax.shard_map(device_fn, mesh=mesh, in_specs=in_specs, out_specs=out_spec, check_vma=False)(acts_in, layer_kind, w_q, w_k, w_v, w_o, w_gate, w_up, w_down, norm_gains, qk_gains)

    return run_all
```

```python
import functools

import jax
import jax.numpy as jnp
from jax import lax
from jax.experimental import pallas as pl
from jax.experimental.pallas import tpu as pltpu
from jax.sharding import PartitionSpec as P


WINDOW = 1024
EPS = 1e-6
LOCAL_BASE = 10000.0
GLOBAL_BASE = 1000000.0
GLOBAL_POS_SCALE = 0.125
CHUNK = 192
LAG = 3
FTILE = 512
KSTEP = 256
NEG = -1e30


def rms_norm(x, gain_vec):
    x_f32 = x.astype(jnp.float32)
    mean_sq = jnp.mean(x_f32 * x_f32, axis=-1, keepdims=True)
    return (x_f32 * lax.rsqrt(mean_sq + EPS) * (1.0 + gain_vec)).astype(jnp.bfloat16)


def rope_tables(kind_val, seq_len, head_dim):
    is_glob = kind_val == 1
    expo_vec = jnp.arange(head_dim // 2, dtype=jnp.float32) * (-2.0 / head_dim)
    inv_freq = jnp.power(jnp.where(is_glob, GLOBAL_BASE, LOCAL_BASE).astype(jnp.float32), expo_vec)
    positions = jnp.arange(seq_len, dtype=jnp.float32) * jnp.where(is_glob, GLOBAL_POS_SCALE, 1.0).astype(jnp.float32)
    angles = positions[:, None] * inv_freq[None, :]
    return jnp.cos(angles), jnp.sin(angles)


def attn_kernel(meta, x_ref, w_ref, wo_ref, kc_ref, vc_ref, cos_ref, sin_ref, gain0_ref, gain_ref, o_ref, ko_ref, vo_ref, h_ref, acc, w_buf, wo_buf, sems, *, n_group, q_scale):
    head = pl.program_id(0)
    kv_heads = w_buf.shape[0]
    cols = w_buf.shape[2]
    o_rows = wo_buf.shape[1]
    cut = cols // 2

    def fetches(h):
        base = h * cols
        if not isinstance(h, int):
            base = pl.multiple_of(base, 128)
        return (
            pltpu.make_async_copy(w_ref.at[:, pl.ds(base, cut)], w_buf.at[h, :, pl.ds(0, cut)], sems.at[h, 0]),
            pltpu.make_async_copy(w_ref.at[:, pl.ds(base + cut, cut)], w_buf.at[h, :, pl.ds(cut, cut)], sems.at[h, 1]),
            pltpu.make_async_copy(wo_ref.at[pl.ds(h * o_rows, o_rows), :], wo_buf.at[h], sems.at[h, 2]),
        )

    @pl.when(head == 0)
    def _():
        for h in range(kv_heads):
            for copy in fetches(h):
                copy.start()

    get_lo, get_hi, get_o = fetches(head)
    chunk = meta[1]
    is_glob = meta[2] == 1
    head_dim = ko_ref.shape[-1]
    half = head_dim // 2
    rows = x_ref.shape[0]
    n_rows = n_group * rows
    cos_b = cos_ref[...]
    sin_b = sin_ref[...]

    @pl.when(head == 0)
    def _():
        x = x_ref[...].astype(jnp.float32)
        mean_sq = jnp.mean(x * x, axis=-1, keepdims=True)
        h_ref[...] = (x * lax.rsqrt(mean_sq + EPS) * (1.0 + gain0_ref[...])).astype(jnp.bfloat16)
        acc[...] = jnp.zeros_like(acc)

    def norm_rope(x, gain):
        x = x.astype(jnp.bfloat16).astype(jnp.float32)
        mean_sq = jnp.mean(x * x, axis=-1, keepdims=True)
        x = x * lax.rsqrt(mean_sq + EPS) * (1.0 + gain)
        lo = x[:, :half]
        hi = x[:, half:]
        return jnp.concatenate([lo * cos_b - hi * sin_b, hi * cos_b + lo * sin_b], axis=-1).astype(jnp.bfloat16)

    get_lo.wait()
    kv_part = jnp.dot(h_ref[...], w_buf[head, :, :cut], preferred_element_type=jnp.float32)
    k_new = norm_rope(kv_part[:, :head_dim], gain_ref[1:2, :])
    v_new = kv_part[:, head_dim:].astype(jnp.bfloat16)
    ko_ref[0, 0] = k_new
    vo_ref[0, 0] = v_new
    get_hi.wait()
    q_part = jnp.dot(h_ref[...], w_buf[head, :, cut:], preferred_element_type=jnp.float32)
    get_o.wait()
    q_all = jnp.concatenate([norm_rope(q_part[:, g * head_dim:(g + 1) * head_dim], gain_ref[0:1, :]) for g in range(n_group)], axis=0)
    start = chunk * rows
    span = jnp.where(is_glob, kc_ref.shape[2], WINDOW)
    first = jnp.where(is_glob, 0, jnp.maximum(start - WINDOW, 0))
    first = pl.multiple_of(first, 64)
    n_old = (start - first + KSTEP - 1) // KSTEP

    dims = (((1,), (1,)), ((), ()))
    dims_pv = (((1,), (0,)), ((), ()))
    s_new = lax.dot_general(q_all, k_new, dims, preferred_element_type=jnp.float32) * q_scale
    q_row = lax.rem(lax.broadcasted_iota(jnp.int32, (n_rows, rows), 0), rows)
    k_col = lax.broadcasted_iota(jnp.int32, (n_rows, rows), 1)
    s_new = jnp.where(k_col <= q_row, s_new, NEG)

    def emit(res):
        res = res.astype(jnp.bfloat16)
        att = jnp.concatenate([res[g * rows:(g + 1) * rows] for g in range(n_group)], axis=1)
        acc[...] += jnp.dot(att, wo_buf[head], preferred_element_type=jnp.float32)

    @pl.when(n_old == 0)
    def _():
        mx = jnp.max(s_new, axis=-1, keepdims=True)
        e_new = jnp.exp(s_new - mx)
        inv = 1.0 / jnp.sum(e_new, axis=-1, keepdims=True)
        emit(lax.dot_general((e_new * inv).astype(jnp.bfloat16), v_new, dims_pv, preferred_element_type=jnp.float32))

    def with_old(n):
        width = n * KSTEP
        k_old = kc_ref[0, 0, pl.ds(first, width), :]
        v_old = vc_ref[0, 0, pl.ds(first, width), :]
        s_old = lax.dot_general(q_all, k_old, dims, preferred_element_type=jnp.float32) * q_scale
        k_pos = first + lax.broadcasted_iota(jnp.int32, (n_rows, width), 1)
        q_pos = start + lax.rem(lax.broadcasted_iota(jnp.int32, (n_rows, width), 0), rows)
        s_old = jnp.where((k_pos < start) & (q_pos - k_pos < span), s_old, NEG)
        mx = jnp.maximum(jnp.max(s_new, axis=-1, keepdims=True), jnp.max(s_old, axis=-1, keepdims=True))
        e_new = jnp.exp(s_new - mx)
        e_old = jnp.exp(s_old - mx)
        inv = 1.0 / (jnp.sum(e_new, axis=-1, keepdims=True) + jnp.sum(e_old, axis=-1, keepdims=True))
        res = lax.dot_general((e_new * inv).astype(jnp.bfloat16), v_new, dims_pv, preferred_element_type=jnp.float32)
        res = res + lax.dot_general((e_old * inv).astype(jnp.bfloat16), v_old, dims_pv, preferred_element_type=jnp.float32)
        emit(res)

    for n in range(1, kc_ref.shape[2] // KSTEP + 1):
        pl.when(n_old == n)(functools.partial(with_old, n))

    @pl.when(head == pl.num_programs(0) - 1)
    def _():
        o_ref[...] = acc[...]


def attend(meta, x, w_qkv, w_o, k_cache, v_cache, cos_tab, sin_tab, gain0, gains, q_scale):
    rows, d_model = x.shape
    _, kv_heads, seq_len, head_dim = k_cache.shape
    cols = w_qkv.shape[1] // kv_heads
    n_group = cols // head_dim - 2
    cache_in = pl.BlockSpec((1, 1, seq_len, head_dim), lambda h, m: (m[0], h, 0, 0))
    cache_out = pl.BlockSpec((1, 1, rows, head_dim), lambda h, m: (m[0], h, m[1], 0))
    table = pl.BlockSpec((rows, head_dim // 2), lambda h, m: (m[1], 0))
    grid_spec = pltpu.PrefetchScalarGridSpec(
        num_scalar_prefetch=1,
        grid=(kv_heads,),
        in_specs=[
            pl.BlockSpec((rows, d_model), lambda h, m: (0, 0)),
            pl.BlockSpec(memory_space=pl.ANY),
            pl.BlockSpec(memory_space=pl.ANY),
            cache_in,
            cache_in,
            table,
            table,
            pl.BlockSpec((1, d_model), lambda h, m: (0, 0)),
            pl.BlockSpec((2, head_dim), lambda h, m: (0, 0)),
        ],
        out_specs=[pl.BlockSpec((rows, d_model), lambda h, m: (0, 0)), cache_out, cache_out],
        scratch_shapes=[
            pltpu.VMEM((rows, d_model), jnp.bfloat16),
            pltpu.VMEM((rows, d_model), jnp.float32),
            pltpu.VMEM((kv_heads, d_model, cols), jnp.bfloat16),
            pltpu.VMEM((kv_heads, n_group * head_dim, d_model), jnp.bfloat16),
            pltpu.SemaphoreType.DMA((kv_heads, 3)),
        ],
    )
    flops = 2 * rows * d_model * (w_qkv.shape[1] + w_o.shape[0]) + 4 * rows * w_o.shape[0] * 900
    return pl.pallas_call(
        functools.partial(attn_kernel, n_group=n_group, q_scale=q_scale),
        grid_spec=grid_spec,
        out_shape=[
            jax.ShapeDtypeStruct((rows, d_model), jnp.float32),
            jax.ShapeDtypeStruct(k_cache.shape, k_cache.dtype),
            jax.ShapeDtypeStruct(v_cache.shape, v_cache.dtype),
        ],
        input_output_aliases={4: 1, 5: 2},
        compiler_params=pltpu.CompilerParams(vmem_limit_bytes=44 * 2**20, dimension_semantics=("arbitrary",)),
        cost_estimate=pl.CostEstimate(flops=flops, bytes_accessed=20 * 2**20, transcendentals=0),
        name="attend",
    )(meta, x, w_qkv, w_o, k_cache, v_cache, cos_tab, sin_tab, gain0, gains)


def mlp_kernel(uo_ref, ux_ref, wg_ref, wu_ref, wd_ref, do_ref, dx_ref, u_all, acc, act):
    step = pl.program_id(0)
    last = pl.num_programs(0) - 1
    rows = uo_ref.shape[0]

    def gate_up():
        gate = jnp.dot(u_all[...], wg_ref[...], preferred_element_type=jnp.float32)
        up = jnp.dot(u_all[...], wu_ref[...], preferred_element_type=jnp.float32)
        return (jax.nn.gelu(gate, approximate=True) * up).astype(jnp.bfloat16)

    def down():
        return jnp.dot(act[...], wd_ref[...], preferred_element_type=jnp.float32)

    @pl.when(step == 0)
    def _():
        u_all[:rows] = uo_ref[...]
        u_all[rows:] = ux_ref[...]
        acc[...] = jnp.zeros_like(acc)
        act[...] = gate_up()

    @pl.when((step > 0) & (step < last))
    def _():
        acc[...] += down()
        act[...] = gate_up()

    @pl.when(step == last)
    def _():
        res = acc[...] + down()
        do_ref[...] = res[:rows]
        dx_ref[...] = res[rows:].astype(jnp.bfloat16)


def mlp(u_own, u_oth, w_gate, w_up, w_down):
    rows, d_model = u_own.shape
    ffn = w_gate.shape[1]
    n_tiles = ffn // FTILE
    whole = pl.BlockSpec((rows, d_model), lambda f: (0, 0))
    col = pl.BlockSpec((d_model, FTILE), lambda f: (0, jnp.minimum(f, n_tiles - 1)))
    row = pl.BlockSpec((FTILE, d_model), lambda f: (jnp.maximum(f - 1, 0), 0))
    return pl.pallas_call(
        mlp_kernel,
        grid=(n_tiles + 1,),
        in_specs=[whole, whole, col, col, row],
        out_specs=[whole, whole],
        out_shape=[jax.ShapeDtypeStruct((rows, d_model), jnp.float32), jax.ShapeDtypeStruct((rows, d_model), jnp.bfloat16)],
        scratch_shapes=[
            pltpu.VMEM((2 * rows, d_model), jnp.bfloat16),
            pltpu.VMEM((2 * rows, d_model), jnp.float32),
            pltpu.VMEM((2 * rows, FTILE), jnp.bfloat16),
        ],
        compiler_params=pltpu.CompilerParams(vmem_limit_bytes=40 * 2**20, dimension_semantics=("arbitrary",)),
        cost_estimate=pl.CostEstimate(flops=12 * rows * d_model * ffn, bytes_accessed=6 * d_model * ffn, transcendentals=0),
        name="mlp",
    )(u_own, u_oth, w_gate, w_up, w_down)


def solution(mesh):
    n_stages = mesh.shape['pp']
    last_stage = n_stages - 1
    col_split = P('pp', None, None, 'tp')
    row_split = P('pp', None, 'tp', None)
    stage_only = P('pp', None, None, None)
    in_specs = (P(None, 'dp', None, None), P('pp', None), col_split, col_split, col_split, row_split, col_split, col_split, row_split, stage_only, stage_only)
    out_spec = P(None, 'dp', 'pp', None)
    axes = ('tp', 'pp')

    def dev(t, s):
        return t * n_stages + s

    def run_all(acts_in, layer_kind, w_q, w_k, w_v, w_o, w_gate, w_up, w_down, norm_gains, qk_gains):
        head_dim = qk_gains.shape[-1]
        q_heads = w_q.shape[-1] // head_dim
        query_pre = acts_in.shape[-1] // q_heads if head_dim == 128 else head_dim
        q_scale = query_pre ** -0.5

        def device_fn(acts_loc, kind_loc, wq_loc, wk_loc, wv_loc, wo_loc, wg_loc, wu_loc, wd_loc, gain_loc, qk_loc):
            side = lax.axis_index('tp')
            stage = lax.axis_index('pp')
            at_first = stage == 0
            n_micro, _, seq_len, d_model = acts_loc.shape
            n_own = n_micro // 2
            n_chunks = seq_len // CHUNK
            n_units = n_own * n_chunks
            kv_heads = wk_loc.shape[-1] // head_dim
            kind_val = kind_loc[0, 0]
            gains = gain_loc[0, 0]
            qk_gain = qk_loc[0, 0]
            w_gate, w_up, w_down = wg_loc[0, 0], wu_loc[0, 0], wd_loc[0, 0]
            f32 = jnp.float32

            def swap(x, stages):
                pairs = [(dev(t, s), dev(1 - t, s)) for s in stages for t in (0, 1)]
                return lax.ppermute(x, axes, pairs)

            n_group = q_heads // (w_k.shape[-1] // head_dim)
            groups = []
            for g in range(kv_heads):
                at_kv = slice(g * head_dim, (g + 1) * head_dim)
                groups += [wk_loc[0, 0][:, at_kv], wv_loc[0, 0][:, at_kv], wq_loc[0, 0][:, g * n_group * head_dim:(g + 1) * n_group * head_dim]]
            wqkv_own = jnp.concatenate(groups, axis=1)
            wo_own = wo_loc[0, 0]
            two = [(wqkv_own, wo_own)]
            got = [(swap(wqkv_own, [s]), swap(wo_own, [s])) for s in range(1, n_stages)]
            cos_tab, sin_tab = rope_tables(kind_val, seq_len, head_dim)
            caches = [jnp.zeros((n_own, kv_heads, seq_len, head_dim), jnp.bfloat16) for _ in range(4)]

            def active(slot):
                return [s for s in range(n_stages) if 0 <= slot - LAG * s < n_units]

            n_slots = n_units + LAG * last_stage
            x_recv, x_mid, u_own, u_oth, d_own, d_oth = {}, {}, {}, {}, {}, {}
            pieces = {}
            landed, landing = [], []
            for slot in range(n_slots + 2):
                if slot < n_slots:
                    unit = jnp.clip(slot - LAG * stage, 0, n_units - 1)
                    meta = jnp.stack([unit % n_own, unit // n_own, kind_val]).astype(jnp.int32)
                    if slot < n_units:
                        row0 = (slot // n_own) * CHUNK
                        at_own = (side * n_own + slot % n_own, 0, row0, 0)
                        at_oth = ((1 - side) * n_own + slot % n_own, 0, row0, 0)
                        size = (1, 1, CHUNK, d_model)
                        x_own = lax.dynamic_slice(acts_loc, at_own, size).reshape(CHUNK, d_model)
                        x_two = lax.dynamic_slice(acts_loc, at_oth, size).reshape(CHUNK, d_model)
                        if slot >= LAG:
                            x_got = lax.optimization_barrier((x_recv[slot], d_own[slot - 2]))[0]
                            x_own = jnp.where(at_first, x_own, x_got)
                            x_two = jnp.where(at_first, x_two, x_got)
                        elif slot >= 2:
                            x_own, x_two, _ = lax.optimization_barrier((x_own, x_two, d_own[slot - 2]))
                    else:
                        x_own = x_two = lax.optimization_barrier((x_recv[slot], d_own[slot - 2]))[0]
                    if slot % LAG == 0 and 0 < slot <= LAG * last_stage:
                        new_qkv, new_o = lax.optimization_barrier((*got[slot // LAG - 1], x_two))[:2]
                        here = stage == slot // LAG
                        two.append((jnp.where(here, new_qkv, two[-1][0]), jnp.where(here, new_o, two[-1][1])))
                    wqkv_two, wo_two = two[-1]
                    o_b, caches[2], caches[3] = attend(meta, x_two, wqkv_two, wo_two, caches[2], caches[3], cos_tab, sin_tab, gains[:1], qk_gain, q_scale)
                    if slot < n_units:
                        o_b = jnp.where(at_first, swap(o_b.astype(jnp.bfloat16), [0]).astype(f32), o_b)
                    o_a, caches[0], caches[1] = attend(meta, x_own, wqkv_own, wo_own, caches[0], caches[1], cos_tab, sin_tab, gains[:1], qk_gain, q_scale)
                    o_sum = (o_a + o_b).astype(jnp.bfloat16)
                    x_mid[slot] = x_own + rms_norm(o_sum, gains[1])
                    u_own[slot] = rms_norm(x_mid[slot], gains[2])
                    u_oth[slot] = swap(u_own[slot], active(slot))
                x_out = None
                if 0 <= slot - 2 < n_slots:
                    done = slot - 2
                    d_mine = d_own[done]
                    if slot < n_slots:
                        d_mine = lax.optimization_barrier((d_mine, o_sum))[0]
                    d_sum = (d_mine + d_oth[done].astype(f32)).astype(jnp.bfloat16)
                    x_out = x_mid[done] + rms_norm(d_sum, gains[3])
                    movers = [s for s in active(done) if s < last_stage]
                    if movers:
                        x_recv[done + LAG] = lax.ppermute(x_out, 'pp', [(s, s + 1) for s in movers])
                    out_unit = done - LAG * last_stage
                    if out_unit >= 0:
                        stream, chunk = out_unit % n_own, out_unit // n_own
                        per = n_chunks // n_stages
                        target, part = chunk // per, chunk % per
                        if target == last_stage:
                            mine = jnp.where(stage == last_stage, x_out, jnp.zeros_like(x_out))
                        else:
                            mine = lax.ppermute(x_out, axes, [(dev(t, last_stage), dev(t, target)) for t in (0, 1)])
                        theirs = lax.ppermute(x_out, axes, [(dev(t, last_stage), dev(1 - t, target)) for t in (0, 1)])
                        for key, val in (((0, stream, part), mine), ((1, stream, part), theirs)):
                            pieces.setdefault(key, []).append(val)
                        landing = [(0, stream, part), (1, stream, part)]

                if 0 <= slot - 1 < n_slots:
                    prev = slot - 1
                    u_in = u_own[prev]
                    if slot < n_slots:
                        u_in = lax.optimization_barrier((u_in, u_own[slot]))[0]
                    if x_out is not None:
                        u_in = lax.optimization_barrier((u_in, x_out))[0]
                    for key in landed:
                        *rest, newest = pieces[key]
                        u_in, newest = lax.optimization_barrier((u_in, newest))
                        pieces[key] = [sum(rest, newest)]
                    d_own[prev], d_send = mlp(u_in, u_oth[prev], w_gate, w_up, w_down)
                    d_oth[prev] = swap(d_send, active(prev))
                landed, landing = landing, []

            per = n_chunks // n_stages
            total = {key: sum(vals[1:], vals[0]) for key, vals in pieces.items()}
            mine = [jnp.concatenate([total[(0, m, r)] for r in range(per)], axis=0) for m in range(n_own)]
            theirs = [jnp.concatenate([total[(1, m, r)] for r in range(per)], axis=0) for m in range(n_own)]
            on_zero = side == 0
            out = [jnp.where(on_zero, a, b) for a, b in zip(mine, theirs)] + [jnp.where(on_zero, b, a) for a, b in zip(mine, theirs)]
            return jnp.stack(out)[:, None]

        return jax.shard_map(device_fn, mesh=mesh, in_specs=in_specs, out_specs=out_spec, check_vma=False)(acts_in, layer_kind, w_q, w_k, w_v, w_o, w_gate, w_up, w_down, norm_gains, qk_gains)

    return run_all
```
